32 devices in a mesh: row: 4 (over y, x), col: 8 (over z, core).
Axes of the slice: x: 2, y: 2, z: 4, core: 2. Of those that a mesh axis runs over, the one named last changes fastest.
Arguments:
- points: bfloat16 [10240, 64], P(('row', 'col')), may hold values from -5 to 5
- start_vectors: bfloat16 [10240, 32], P(('row', 'col')), may hold values from -12 to 12
Outputs:
- basis: float32 [10240, 32], P(('row', 'col'))
The draws below stay inside these ranges and needn't reach their ends.
All inputs are finite; a program needn't handle non-finite values.
Results may differ from the reference program's by a relative error of at most 0.007.
Values may be sent and summed in bfloat16 or wider, within the bound.
A program may use at most 64 MiB of HBM per device.

```python
import jax
import jax.numpy as jnp
from jax import lax

F = 64
K = 32
ITERS = 2
PTS_BLK = 2560
POINTS = 10240


def draw_points(key, part):
    order_key, center_key, noise_key, sigma_key = jax.random.split(jax.random.fold_in(key, 11), 4)
    pairs = POINTS // 2
    order = jax.random.permutation(order_key, POINTS)
    pair_of = jnp.zeros((POINTS,), jnp.int32).at[order].set(jnp.arange(POINTS, dtype=jnp.int32) // 2)
    sigma = jnp.exp(jax.random.uniform(sigma_key, (pairs, 1), jnp.float32, jnp.log(0.15), jnp.log(0.4)))
    centers = jnp.clip(jax.random.normal(center_key, (pairs, F), jnp.float32), -4.0, 4.0)
    noise = jnp.clip(jax.random.normal(noise_key, (POINTS, F), jnp.float32), -3.0, 3.0)
    values = centers[pair_of] + sigma[pair_of] * noise
    return jnp.clip(values, -5.0, 5.0).astype(jnp.bfloat16)


def draw_start_vectors(key, part):
    position = jnp.arange(POINTS, dtype=jnp.float32)[:, None] / POINTS
    base = jnp.clip(jax.random.normal(key, (POINTS, K), jnp.float32), -3.0, 3.0)
    values = base * jnp.exp(jnp.log(4.0) * position)
    return jnp.clip(values, -12.0, 12.0).astype(jnp.bfloat16)


def setup_inputs(seed: int = 0) -> dict:
    key_of = jax.random.split(jax.random.key(seed), 3)
    return {
        "points": draw_points(jax.random.fold_in(key_of[2], 71), 0),
        "start_vectors": draw_start_vectors(jax.random.fold_in(key_of[2], 71), 0),
    }


KERNEL_SCALE = 5.12

def kernel_block(block_pts, block_sq, all_pts, all_sq):
    cross = jnp.dot(block_pts.astype(jnp.float32), all_pts.T.astype(jnp.float32), preferred_element_type=jnp.float32)
    dist = block_sq[:, None] + all_sq[None, :] - 2.0 * cross
    return jnp.exp(dist * (-KERNEL_SCALE / F)).astype(jnp.bfloat16)

def reference(points, start_vectors):
    sq_norms = jnp.sum(jnp.square(points.astype(jnp.float32)), axis=1)
    height = min(512, PTS_BLK)
    count = POINTS // height
    stacked = (points.reshape(count, height, F), sq_norms.reshape(count, height))

    def degree_block(item):
        weights = kernel_block(item[0], item[1], points, sq_norms)
        return jnp.sum(weights, axis=1, dtype=jnp.float32)
    degree = lax.map(degree_block, stacked).reshape(POINTS)
    vectors = start_vectors
    ortho = jnp.zeros((POINTS, K), jnp.float32)
    for step in range(ITERS):

        def product_block(item, panel=vectors):
            weights = kernel_block(item[0], item[1], points, sq_norms)
            return jnp.dot(weights.astype(jnp.float32), panel.astype(jnp.float32), preferred_element_type=jnp.float32)
        product = lax.map(product_block, stacked).reshape(POINTS, K)
        scaled = product / degree[:, None]
        gram = jnp.dot(scaled.T.astype(jnp.float32), scaled.astype(jnp.float32), precision=lax.Precision.HIGHEST, preferred_element_type=jnp.float32) / POINTS
        lower = jnp.linalg.cholesky(gram)
        ortho = lax.linalg.triangular_solve(lower, scaled, left_side=False, lower=True, transpose_a=True)
        vectors = ortho.astype(jnp.bfloat16)
    return ortho
```

```python
import functools

import jax
import jax.numpy as jnp
from jax import lax
from jax.experimental import pallas as pl
from jax.experimental.pallas import tpu as pltpu
from jax.sharding import PartitionSpec as P

KERNEL_SCALE = 5.12
LOG2E = 1.4426950408889634
MESH = pl.DeviceIdType.MESH
HIGHEST = lax.Precision.HIGHEST
LANES = 128


def packing(rows):
    for stacks in (4, 2, 1):
        if rows % (16 * stacks) == 0:
            return stacks
    raise ValueError(rows)


def width(stacks, lanes):
    return -(-stacks * lanes // LANES) * LANES


def side_by_side(value, stacks):
    rows, lanes = value.shape
    high = rows // stacks
    pieces = [value[s * high : (s + 1) * high] for s in range(stacks)]
    spare = width(stacks, lanes) - stacks * lanes
    if spare:
        pieces.append(jnp.zeros((high, spare), value.dtype))
    return jnp.concatenate(pieces, axis=1)


def inverse_factor(gram):
    size = gram.shape[0]
    down = lax.broadcasted_iota(jnp.int32, (size, size), 0)
    across = lax.broadcasted_iota(jnp.int32, (size, size), 1)
    unit = (down == across).astype(jnp.float32)
    work = jnp.concatenate([gram, unit], axis=1)
    below = lax.broadcasted_iota(jnp.int32, (size, 1), 0)
    for k in range(size - 1):
        row = work[k : k + 1, :]
        factor = work[:, k : k + 1] * (1.0 / work[k : k + 1, k : k + 1])
        work = work - jnp.where(below > k, factor, 0.0) * row
    pivots = jnp.sum(work[:, :size] * unit, axis=1, keepdims=True)
    return work[:, size:] * lax.rsqrt(pivots)


def kernel(nrow, ncol, total, pts_ref, vec_ref, out_ref, gp, gv, gs, aff, acc,
           gram_col, gram_row, sems_p, sems_v, sems_s, sems_g):
    row, col = lax.axis_index("row"), lax.axis_index("col")
    nz = ncol // 2
    z, core = col // 2, col % 2
    sibling = z * 2 + (1 - core)
    rows, features = pts_ref.shape
    vectors = vec_ref.shape[1]
    stacks = packing(rows)
    high = rows // stacks
    per_tile = max(1, LANES // features)

    def row_at(j):
        return lax.rem(row + j, nrow)

    def col_at(k):
        return lax.rem(z + k, nz) * 2 + core

    def view(buf, r, c):
        return buf.at[r, pl.ds(pl.multiple_of(c * high, high), high)]

    def block(buf, r, c, send, recv, to_row, to_col):
        return pltpu.make_async_remote_copy(
            src_ref=view(buf, r, c), dst_ref=view(buf, r, c), send_sem=send, recv_sem=recv.at[r, c],
            device_id=(to_row, to_col), device_id_type=MESH,
        )

    def arrived(gather, r, c):
        buf, recv, along, spread, pair = gather
        block(buf, r, c, pair.at[0, 0], recv, row, sibling).wait_recv()

    def hand_over(gather, j, k):
        buf, recv, along, spread, pair = gather
        block(buf, row_at(j), col_at(k), pair.at[j, k], recv, row, sibling).start()

    def send_plane(gather, k):
        buf, recv, along, spread, pair = gather
        for j in range(1, nrow):
            block(buf, row, col_at(k), spread.at[k, j - 1], recv, row_at(j), col).start()
        hand_over(gather, 0, k)

    def send_own(gather):
        buf, recv, along, spread, pair = gather
        for k in range(1, nz):
            block(buf, row, col, along.at[k - 1], recv, row, col_at(k)).start()
        send_plane(gather, 0)

    def pass_on(gather):
        for k in range(1, nz):
            arrived(gather, row, col_at(k))
            send_plane(gather, k)

    def hand_over_row(gather, j):
        for k in range(nz):
            arrived(gather, row_at(j), col_at(k))
            hand_over(gather, j, k)

    def sibling_row(gather, j):
        for k in range(nz):
            arrived(gather, row_at(j), lax.rem(z + k, nz) * 2 + (1 - core))

    def drain(gather):
        buf, recv, along, spread, pair = gather
        for k in range(1, nz):
            block(buf, row, col, along.at[k - 1], recv, row, col_at(k)).wait_send()
        for k in range(nz):
            for j in range(1, nrow):
                block(buf, row, col_at(k), spread.at[k, j - 1], recv, row_at(j), col).wait_send()
            for j in range(nrow):
                block(buf, row_at(j), col_at(k), pair.at[j, k], recv, row, sibling).wait_send()

    points = (gp,) + tuple(sems_p)
    start = (gv,) + tuple(sems_v)
    middle = (gs,) + tuple(sems_s)

    barrier = pltpu.get_barrier_semaphore()
    for j in range(1, nrow):
        pl.semaphore_signal(barrier, inc=1, device_id=(row_at(j), col), device_id_type=MESH)
    for k in range(1, ncol):
        pl.semaphore_signal(barrier, inc=1, device_id=(row, lax.rem(col + k, ncol)), device_id_type=MESH)

    own = pl.ds(pl.multiple_of(col * high, high), high)
    x = pts_ref[...]
    gp[row, own, :] = side_by_side(x, stacks)
    gv[row, own, :] = side_by_side(vec_ref[...], stacks)
    pl.semaphore_wait(barrier, nrow + ncol - 2)

    send_own(points)
    send_own(start)

    rate = -KERNEL_SCALE / features * LOG2E
    xf = x.astype(jnp.float32)
    here = jnp.sum(xf * xf, axis=1, keepdims=True) * rate
    blank = jnp.zeros_like(x)
    left = []
    for s in range(per_tile):
        parts = [x if s == t else blank for t in range(per_tile)]
        left.append(jnp.concatenate(parts, axis=1))
    lane = lax.broadcasted_iota(jnp.int32, (8 * per_tile, LANES), 1)
    down = lax.broadcasted_iota(jnp.int32, (8 * per_tile, LANES), 0)
    picks = (lane // features == down // 8).astype(jnp.bfloat16)
    contract = (((1,), (1,)), ((), ()))

    def weights(r):
        for s in range(stacks):
            tile, part = s // per_tile, s % per_tile
            right = gp[r, :, tile * LANES : (tile + 1) * LANES]
            if part == 0:
                wide = right.astype(jnp.float32)
                square = wide * wide
                upper = square.astype(jnp.bfloat16)
                lower = (square - upper.astype(jnp.float32)).astype(jnp.bfloat16)
                there = (
                    lax.dot_general(picks, upper, contract, preferred_element_type=jnp.float32)
                    + lax.dot_general(picks, lower, contract, preferred_element_type=jnp.float32)
                ) * rate
            cross = lax.dot_general(left[part], right, contract, preferred_element_type=jnp.float32)
            power = (cross * (-2.0 * rate) + there[8 * part : 8 * part + 1]) + here
            aff[r, s] = jnp.exp2(power).astype(jnp.bfloat16)

    pass_on(points)
    pass_on(start)
    sibling_row(points, 0)
    weights(row)

    def next_row(j, carry):
        hand_over_row(points, j)
        sibling_row(points, j)
        weights(row_at(j))
        return carry

    lax.fori_loop(1, nrow, next_row, 0)

    span = gv.shape[2]
    ones = jnp.ones((ncol * high, LANES), jnp.bfloat16)
    acc[...] = jnp.zeros_like(acc)

    def first_row(j, carry):
        sibling_row(start, j)
        r = row_at(j)
        panel = jnp.concatenate([gv[r], ones], axis=1)
        for s in range(stacks):
            acc[s] += jnp.dot(aff[r, s], panel, preferred_element_type=jnp.float32)
        return carry

    def hand_over_start(j, carry):
        hand_over_row(start, j)
        return carry

    lax.fori_loop(1, nrow, hand_over_start, 0)
    lax.fori_loop(0, nrow, first_row, 0)

    product = sum(acc[s][:, s * vectors : (s + 1) * vectors] for s in range(stacks))
    degree = sum(acc[s][:, span : span + vectors] for s in range(stacks))
    scaled = product / degree
    gs[row, own, :] = side_by_side(scaled.astype(jnp.bfloat16), stacks)
    send_own(middle)

    folds = LANES // vectors
    tall = vectors // folds

    def gram_send(step, value):
        part = jnp.dot(value.T, value, precision=HIGHEST, preferred_element_type=jnp.float32) * (1.0 / total)
        gram_col[step, col] = jnp.concatenate([part[f * tall : (f + 1) * tall] for f in range(folds)], axis=1)
        for k in range(1, ncol):
            gram_copy(gram_col, step, col, k - 1, row, lax.rem(col + k, ncol), 0).start()

    def gram_copy(buf, step, slot, k, to_row, to_col, axis):
        return pltpu.make_async_remote_copy(
            src_ref=buf.at[step, slot], dst_ref=buf.at[step, slot],
            send_sem=sems_g[2 * axis].at[step, k], recv_sem=sems_g[2 * axis + 1].at[step, slot],
            device_id=(to_row, to_col), device_id_type=MESH,
        )

    def gram_across(step):
        for k in range(1, ncol):
            slot = lax.rem(col + k, ncol)
            gram_copy(gram_col, step, slot, k - 1, row, slot, 0).wait_recv()
        gram_row[step, row] = sum(gram_col[step, c] for c in range(ncol))
        for j in range(1, nrow):
            gram_copy(gram_row, step, row, j - 1, row_at(j), col, 1).start()

    def gram_whole(step):
        for j in range(1, nrow):
            gram_copy(gram_row, step, row_at(j), j - 1, row_at(j), col, 1).wait_recv()
        flat = sum(gram_row[step, r] for r in range(nrow))
        return jnp.concatenate([flat[:, f * vectors : (f + 1) * vectors] for f in range(folds)], axis=0)

    def gram_drain(step):
        for k in range(1, ncol):
            gram_copy(gram_col, step, col, k - 1, row, lax.rem(col + k, ncol), 0).wait_send()
        for j in range(1, nrow):
            gram_copy(gram_row, step, row, j - 1, row_at(j), col, 1).wait_send()

    gram_send(0, scaled)
    pass_on(middle)
    gram_across(0)
    first = inverse_factor(gram_whole(0))

    def hand_over_middle(j, carry):
        hand_over_row(middle, j)
        return carry

    def second_row(j, carry):
        sibling_row(middle, j)
        r = row_at(j)
        for s in range(stacks):
            acc[s, :, :span] += jnp.dot(aff[r, s], gs[r], preferred_element_type=jnp.float32)
        return carry

    acc[...] = jnp.zeros_like(acc)
    lax.fori_loop(1, nrow, hand_over_middle, 0)
    lax.fori_loop(0, nrow, second_row, 0)
    product = sum(acc[s][:, s * vectors : (s + 1) * vectors] for s in range(stacks))
    scaled = lax.dot_general(
        product / degree, first, contract, precision=HIGHEST, preferred_element_type=jnp.float32
    )
    gram_send(1, scaled)
    drain(points)
    drain(start)
    drain(middle)
    gram_drain(0)
    gram_across(1)
    second = inverse_factor(gram_whole(1))
    out_ref[...] = lax.dot_general(scaled, second, contract, precision=HIGHEST, preferred_element_type=jnp.float32)
    gram_drain(1)


def solution(mesh):
    nrow, ncol = mesh.shape["row"], mesh.shape["col"]
    nz = ncol // 2

    def step(points, start_vectors):
        rows, features = points.shape
        vectors = start_vectors.shape[1]
        stacks = packing(rows)
        high = rows // stacks
        wide, span = width(stacks, features), width(stacks, vectors)
        dma = pltpu.SemaphoreType.DMA
        gather = [dma((nrow, ncol)), dma((nz,)), dma((nz, nrow)), dma((nrow, nz))]
        tall = vectors * vectors // LANES
        return pl.pallas_call(
            functools.partial(kernel, nrow, ncol, rows * nrow * ncol),
            out_shape=jax.ShapeDtypeStruct((rows, vectors), jnp.float32),
            in_specs=[pl.BlockSpec(memory_space=pltpu.VMEM)] * 2,
            out_specs=pl.BlockSpec(memory_space=pltpu.VMEM),
            scratch_shapes=[
                pltpu.VMEM((nrow, ncol * high, wide), jnp.bfloat16),
                pltpu.VMEM((nrow, ncol * high, span), jnp.bfloat16),
                pltpu.VMEM((nrow, ncol * high, span), jnp.bfloat16),
                pltpu.VMEM((nrow, stacks, rows, ncol * high), jnp.bfloat16),
                pltpu.VMEM((stacks, rows, span + LANES), jnp.float32),
                pltpu.VMEM((2, ncol, tall, LANES), jnp.float32),
                pltpu.VMEM((2, nrow, tall, LANES), jnp.float32),
                gather, gather, gather,
                [dma((2, ncol)), dma((2, ncol)), dma((2, nrow)), dma((2, nrow))],
            ],
            compiler_params=pltpu.CompilerParams(
                collective_id=0, has_side_effects=True, vmem_limit_bytes=56 * 1024 * 1024
            ),
        )(points, start_vectors)

    return jax.shard_map(
        step,
        mesh=mesh,
        in_specs=(P(("row", "col"), None), P(("row", "col"), None)),
        out_specs=P(("row", "col"), None),
        check_vma=False,
    )
```

```python
import functools

import jax
import jax.numpy as jnp
from jax import lax
from jax.experimental import pallas as pl
from jax.experimental.pallas import tpu as pltpu
from jax.sharding import PartitionSpec as P

KERNEL_SCALE = 5.12
LOG2E = 1.4426950408889634
MESH = pl.DeviceIdType.MESH
HIGHEST = lax.Precision.HIGHEST
LANES = 128


def packing(rows):
    for stacks in (4, 2, 1):
        if rows % (16 * stacks) == 0:
            return stacks
    raise ValueError(rows)


def square_side(count):
    side = 1
    while side * side < count:
        side += 1
    return side if side * side == count else count


def upright(value):
    return value.astype(jnp.float32).T.astype(value.dtype)


def width(stacks, lanes):
    return -(-stacks * lanes // LANES) * LANES


def side_by_side(value, stacks):
    rows, lanes = value.shape
    high = rows // stacks
    pieces = [value[s * high : (s + 1) * high] for s in range(stacks)]
    spare = width(stacks, lanes) - stacks * lanes
    if spare:
        pieces.append(jnp.zeros((high, spare), value.dtype))
    return jnp.concatenate(pieces, axis=1)


def inverse_factor(gram):
    size = gram.shape[0]
    down = lax.broadcasted_iota(jnp.int32, (size, size), 0)
    across = lax.broadcasted_iota(jnp.int32, (size, size), 1)
    unit = (down == across).astype(jnp.float32)
    work = jnp.concatenate([gram, unit], axis=1)
    below = lax.broadcasted_iota(jnp.int32, work.shape, 0)
    panel = 8
    for first in range(0, size, panel):
        columns = [jnp.broadcast_to(work[:, k : k + 1], work.shape) for k in range(first, first + panel)]
        for m in range(panel):
            k = first + m
            factor = jnp.where(below > k, columns[m] * (1.0 / columns[m][k : k + 1]), 0.0)
            work = work - factor * work[k : k + 1]
            for later in range(m + 1, panel):
                columns[later] = columns[later] - factor * columns[later][k : k + 1]
    pivots = jnp.sum(work[:, :size] * unit, axis=1, keepdims=True)
    return work[:, size:] * lax.rsqrt(pivots)


def kernel(nrow, ncol, total, pts_ref, vec_ref, out_ref, gp, gv, gs, aff, acc,
           gram_col, gram_row, sems_p, sems_v, sems_s, sems_g):
    row, col = lax.axis_index("row"), lax.axis_index("col")
    nz = ncol // 2
    z, core = col // 2, col % 2
    sibling = z * 2 + (1 - core)
    features, rows = pts_ref.shape
    vectors = vec_ref.shape[0]
    side = square_side(nrow)
    high_row, low_row = row // side, row % side
    stacks = packing(rows)
    high = rows // stacks
    per_tile = max(1, LANES // features)

    def row_at(j):
        return lax.rem(high_row + j // side, nrow // side) * side + lax.rem(low_row + j % side, side)

    straight = [j for j in range(1, nrow) if j // side == 0 or j % side == 0]
    oblique = [j for j in range(1, nrow) if j // side and j % side]

    def col_at(k):
        return lax.rem(z + k, nz) * 2 + core

    def view(buf, r, c):
        return buf.at[r, pl.ds(pl.multiple_of(c * high, high), high)]

    def block(buf, r, c, send, recv, to_row, to_col):
        return pltpu.make_async_remote_copy(
            src_ref=view(buf, r, c), dst_ref=view(buf, r, c), send_sem=send, recv_sem=recv.at[r, c],
            device_id=(to_row, to_col), device_id_type=MESH,
        )

    def arrived(gather, r, c):
        buf, recv, along, spread, pair, onward, routed = gather
        block(buf, r, c, pair.at[0, 0], recv, row, sibling).wait_recv()

    def hand_over(gather, j, k):
        buf, recv, along, spread, pair, onward, routed = gather
        block(buf, row_at(j), col_at(k), pair.at[j, k], recv, row, sibling).start()

    def send_plane(gather, k):
        buf, recv, along, spread, pair, onward, routed = gather
        for j in straight + (oblique if routed else []):
            block(buf, row, col_at(k), spread.at[k, j], recv, row_at(j), col).start()
        hand_over(gather, 0, k)

    def relays(gather, j, k):
        buf, recv, along, spread, pair, onward, routed = gather
        copies = []
        if routed:
            targets = []
        elif j // side == 0 and k % 2 == 0:
            targets = [d * side for d in range(1, nrow // side)]
        elif j % side == 0 and k % 2 == 1:
            targets = range(1, side)
        else:
            targets = []
        return [
            block(buf, row_at(j), col_at(k), onward.at[j, k, i], recv, row_at(t), col)
            for i, t in enumerate(targets)
        ]

    def relay(gather, k):
        for j in straight:
            arrived(gather, row_at(j), col_at(k))
            for copy in relays(gather, j, k):
                copy.start()
            hand_over(gather, j, k)

    def send_own(gather):
        buf, recv, along, spread, pair, onward, routed = gather
        for k in range(1, nz):
            block(buf, row, col, along.at[k - 1], recv, row, col_at(k)).start()
        send_plane(gather, 0)

    def pass_on(gather, k):
        arrived(gather, row, col_at(k))
        send_plane(gather, k)

    def hand_over_row(gather, j):
        for k in range(nz):
            arrived(gather, row_at(j), col_at(k))
            hand_over(gather, j, k)

    def sibling_row(gather, j):
        for k in range(nz):
            arrived(gather, row_at(j), lax.rem(z + k, nz) * 2 + (1 - core))

    def drain(gather):
        buf, recv, along, spread, pair, onward, routed = gather
        for k in range(1, nz):
            block(buf, row, col, along.at[k - 1], recv, row, col_at(k)).wait_send()
        for k in range(nz):
            for j in straight + (oblique if routed else []):
                block(buf, row, col_at(k), spread.at[k, j], recv, row_at(j), col).wait_send()
                for copy in relays(gather, j, k):
                    copy.wait_send()
            for j in range(nrow):
                block(buf, row_at(j), col_at(k), pair.at[j, k], recv, row, sibling).wait_send()

    points = (gp,) + tuple(sems_p) + (False,)
    start = (gv,) + tuple(sems_v) + (False,)
    middle = (gs,) + tuple(sems_s) + (True,)

    barrier = pltpu.get_barrier_semaphore()
    for j in range(1, nrow):
        pl.semaphore_signal(barrier, inc=1, device_id=(row_at(j), col), device_id_type=MESH)
    for k in range(1, ncol):
        pl.semaphore_signal(barrier, inc=1, device_id=(row, lax.rem(col + k, ncol)), device_id_type=MESH)

    own = pl.ds(pl.multiple_of(col * high, high), high)
    x = upright(pts_ref[...])
    gp[row, own, :] = side_by_side(x, stacks)
    gv[row, own, :] = side_by_side(upright(vec_ref[...]), stacks)
    pl.semaphore_wait(barrier, nrow + ncol - 2)

    send_own(points)
    send_own(start)

    rate = -KERNEL_SCALE / features * LOG2E
    xf = x.astype(jnp.float32)
    here = jnp.sum(xf * xf, axis=1, keepdims=True) * rate
    blank = jnp.zeros_like(x)
    left = []
    for s in range(per_tile):
        parts = [x if s == t else blank for t in range(per_tile)]
        left.append(jnp.concatenate(parts, axis=1))
    lane = lax.broadcasted_iota(jnp.int32, (8 * per_tile, LANES), 1)
    down = lax.broadcasted_iota(jnp.int32, (8 * per_tile, LANES), 0)
    picks = (lane // features == down // 8).astype(jnp.bfloat16)
    contract = (((1,), (1,)), ((), ()))

    def weights(r):
        for s in range(stacks):
            tile, part = s // per_tile, s % per_tile
            right = gp[r, :, tile * LANES : (tile + 1) * LANES]
            if part == 0:
                wide = right.astype(jnp.float32)
                square = wide * wide
                upper = square.astype(jnp.bfloat16)
                lower = (square - upper.astype(jnp.float32)).astype(jnp.bfloat16)
                there = (
                    lax.dot_general(picks, upper, contract, preferred_element_type=jnp.float32)
                    + lax.dot_general(picks, lower, contract, preferred_element_type=jnp.float32)
                ) * rate
            cross = lax.dot_general(left[part], right, contract, preferred_element_type=jnp.float32)
            power = (cross * (-2.0 * rate) + there[8 * part : 8 * part + 1]) + here
            aff[r, s] = jnp.exp2(power).astype(jnp.bfloat16)

    for k in range(1, nz):
        pass_on(points, k)
        pass_on(start, k)
        relay(points, k - 1)
    relay(points, nz - 1)
    sibling_row(points, 0)
    weights(row)
    for k in range(nz):
        relay(start, k)
    for j in straight:
        sibling_row(points, j)
        weights(row_at(j))
        if j == straight[0]:
            for o in oblique:
                hand_over_row(points, o)
    for j in oblique:
        sibling_row(points, j)
        weights(row_at(j))

    span = gv.shape[2]
    ones = jnp.ones((ncol * high, LANES), jnp.bfloat16)
    acc[...] = jnp.zeros_like(acc)

    def first_row(j):
        sibling_row(start, j)
        r = row_at(j)
        panel = jnp.concatenate([gv[r], ones], axis=1)
        for s in range(stacks):
            acc[s] += jnp.dot(aff[r, s], panel, preferred_element_type=jnp.float32)

    for j in [0] + straight:
        first_row(j)
    for j in oblique:
        hand_over_row(start, j)
    for j in oblique:
        first_row(j)

    product = sum(acc[s][:, s * vectors : (s + 1) * vectors] for s in range(stacks))
    degree = sum(acc[s][:, span : span + vectors] for s in range(stacks))
    scaled = product / degree
    gs[row, own, :] = side_by_side(scaled.astype(jnp.bfloat16), stacks)
    send_own(middle)

    folds = LANES // vectors
    tall = vectors // folds

    def gram_send(step, value):
        part = jnp.dot(value.T, value, precision=HIGHEST, preferred_element_type=jnp.float32) * (1.0 / total)
        gram_col[step, col] = jnp.concatenate([part[f * tall : (f + 1) * tall] for f in range(folds)], axis=1)
        for k in range(1, ncol):
            gram_copy(gram_col, step, col, k - 1, row, lax.rem(col + k, ncol), 0).start()

    def gram_copy(buf, step, slot, k, to_row, to_col, axis):
        return pltpu.make_async_remote_copy(
            src_ref=buf.at[step, slot], dst_ref=buf.at[step, slot],
            send_sem=sems_g[2 * axis].at[step, k], recv_sem=sems_g[2 * axis + 1].at[step, slot],
            device_id=(to_row, to_col), device_id_type=MESH,
        )

    def gram_across(step):
        for k in range(1, ncol):
            slot = lax.rem(col + k, ncol)
            gram_copy(gram_col, step, slot, k - 1, row, slot, 0).wait_recv()
        gram_row[step, row] = sum(gram_col[step, c] for c in range(ncol))
        for j in range(1, nrow):
            gram_copy(gram_row, step, row, j - 1, row_at(j), col, 1).start()

    def gram_whole(step):
        for j in range(1, nrow):
            gram_copy(gram_row, step, row_at(j), j - 1, row_at(j), col, 1).wait_recv()
        flat = sum(gram_row[step, r] for r in range(nrow))
        return jnp.concatenate([flat[:, f * vectors : (f + 1) * vectors] for f in range(folds)], axis=0)

    def gram_drain(step):
        for k in range(1, ncol):
            gram_copy(gram_col, step, col, k - 1, row, lax.rem(col + k, ncol), 0).wait_send()
        for j in range(1, nrow):
            gram_copy(gram_row, step, row, j - 1, row_at(j), col, 1).wait_send()

    for k in range(1, nz):
        pass_on(middle, k)
        relay(middle, k - 1)
    relay(middle, nz - 1)
    mixed = jnp.zeros((span, span), jnp.float32)
    acc[...] = jnp.zeros_like(acc)

    def second_row(j):
        sibling_row(middle, j)
        r = row_at(j)
        for s in range(stacks):
            acc[s, :, :span] += jnp.dot(aff[r, s], gs[r], preferred_element_type=jnp.float32)
        return mixed + jnp.dot(upright(gs[r]), gs[r], preferred_element_type=jnp.float32)

    for j in [0] + straight:
        mixed = second_row(j)
    for j in oblique:
        hand_over_row(middle, j)
    for j in oblique:
        mixed = second_row(j)
    gram = sum(
        mixed[s * vectors : (s + 1) * vectors, s * vectors : (s + 1) * vectors] for s in range(stacks)
    )
    first = inverse_factor(gram * (1.0 / total))
    product = sum(acc[s][:, s * vectors : (s + 1) * vectors] for s in range(stacks))
    scaled = lax.dot_general(
        product / degree, first, contract, precision=HIGHEST, preferred_element_type=jnp.float32
    )
    gram_send(0, scaled)
    drain(points)
    drain(start)
    drain(middle)
    gram_across(0)
    second = inverse_factor(gram_whole(0))
    out_ref[...] = lax.dot_general(second, scaled, contract, precision=HIGHEST, preferred_element_type=jnp.float32)
    gram_drain(0)


def solution(mesh):
    nrow, ncol = mesh.shape["row"], mesh.shape["col"]
    nz = ncol // 2

    def step(points, start_vectors):
        rows, features = points.shape
        vectors = start_vectors.shape[1]
        stacks = packing(rows)
        high = rows // stacks
        wide, span = width(stacks, features), width(stacks, vectors)
        dma = pltpu.SemaphoreType.DMA
        gather = [dma((nrow, ncol)), dma((nz,)), dma((nz, nrow)), dma((nrow, nz)), dma((nrow, nz, square_side(nrow)))]
        tall = vectors * vectors // LANES
        return pl.pallas_call(
            functools.partial(kernel, nrow, ncol, rows * nrow * ncol),
            out_shape=jax.ShapeDtypeStruct((vectors, rows), jnp.float32),
            in_specs=[pl.BlockSpec(memory_space=pltpu.VMEM)] * 2,
            out_specs=pl.BlockSpec(memory_space=pltpu.VMEM),
            scratch_shapes=[
                pltpu.VMEM((nrow, ncol * high, wide), jnp.bfloat16),
                pltpu.VMEM((nrow, ncol * high, span), jnp.bfloat16),
                pltpu.VMEM((nrow, ncol * high, span), jnp.bfloat16),
                pltpu.VMEM((nrow, stacks, rows, ncol * high), jnp.bfloat16),
                pltpu.VMEM((stacks, rows, span + LANES), jnp.float32),
                pltpu.VMEM((1, ncol, tall, LANES), jnp.float32),
                pltpu.VMEM((1, nrow, tall, LANES), jnp.float32),
                gather, gather, gather,
                [dma((1, ncol)), dma((1, ncol)), dma((1, nrow)), dma((1, nrow))],
            ],
            compiler_params=pltpu.CompilerParams(
                collective_id=0, has_side_effects=True, vmem_limit_bytes=56 * 1024 * 1024
            ),
        )(points.T, start_vectors.T).T

    return jax.shard_map(
        step,
        mesh=mesh,
        in_specs=(P(("row", "col"), None), P(("row", "col"), None)),
        out_specs=P(("row", "col"), None),
        check_vma=False,
    )
```

```python
import functools

import jax
import jax.numpy as jnp
from jax import lax
from jax.experimental import pallas as pl
from jax.experimental.pallas import tpu as pltpu
from jax.sharding import PartitionSpec as P

KERNEL_SCALE = 5.12
LOG2E = 1.4426950408889634
MESH = pl.DeviceIdType.MESH
HIGHEST = lax.Precision.HIGHEST
LANES = 128


def packing(rows):
    for stacks in (4, 2, 1):
        if rows % (16 * stacks) == 0:
            return stacks
    raise ValueError(rows)


def square_side(count):
    side = 1
    while side * side < count:
        side += 1
    return side if side * side == count else count


def upright(value):
    return value.astype(jnp.float32).T.astype(value.dtype)


def width(stacks, lanes):
    return -(-stacks * lanes // LANES) * LANES


def side_by_side(value, stacks):
    rows, lanes = value.shape
    high = rows // stacks
    pieces = [value[s * high : (s + 1) * high] for s in range(stacks)]
    spare = width(stacks, lanes) - stacks * lanes
    if spare:
        pieces.append(jnp.zeros((high, spare), value.dtype))
    return jnp.concatenate(pieces, axis=1)


def inverse_factor(gram):
    size = gram.shape[0]
    down = lax.broadcasted_iota(jnp.int32, (size, size), 0)
    across = lax.broadcasted_iota(jnp.int32, (size, size), 1)
    unit = (down == across).astype(jnp.float32)
    work = jnp.concatenate([gram, unit], axis=1)
    below = lax.broadcasted_iota(jnp.int32, work.shape, 0)
    panel = 8
    for first in range(0, size, panel):
        columns = [jnp.broadcast_to(work[:, k : k + 1], work.shape) for k in range(first, first + panel)]
        for m in range(panel):
            k = first + m
            factor = jnp.where(below > k, columns[m] * (1.0 / columns[m][k : k + 1]), 0.0)
            work = work - factor * work[k : k + 1]
            for later in range(m + 1, panel):
                columns[later] = columns[later] - factor * columns[later][k : k + 1]
    pivots = jnp.sum(work[:, :size] * unit, axis=1, keepdims=True)
    return work[:, size:] * lax.rsqrt(pivots)


def kernel(nrow, ncol, total, pts_ref, vec_ref, out_ref, gp, gv, gs, aff, acc,
           gram_col, gram_row, sems_p, sems_v, sems_s, sems_g):
    row, col = lax.axis_index("row"), lax.axis_index("col")
    nz = ncol // 2
    z, core = col // 2, col % 2
    sibling = z * 2 + (1 - core)
    features, rows = pts_ref.shape
    vectors = vec_ref.shape[0]
    side = square_side(nrow)
    high_row, low_row = row // side, row % side
    stacks = packing(rows)
    high = rows // stacks
    per_tile = max(1, LANES // features)

    def row_at(j):
        return lax.rem(high_row + j // side, nrow // side) * side + lax.rem(low_row + j % side, side)

    straight = [j for j in range(1, nrow) if j // side == 0 or j % side == 0]
    oblique = [j for j in range(1, nrow) if j // side and j % side]

    def col_at(k):
        return lax.rem(z + k, nz) * 2 + core

    def view(buf, r, c):
        return buf.at[r, pl.ds(pl.multiple_of(c * high, high), high)]

    def block(buf, r, c, send, recv, to_row, to_col):
        return pltpu.make_async_remote_copy(
            src_ref=view(buf, r, c), dst_ref=view(buf, r, c), send_sem=send, recv_sem=recv.at[r, c],
            device_id=(to_row, to_col), device_id_type=MESH,
        )

    def arrived(gather, r, c):
        buf, recv, along, spread, pair, onward, routed = gather
        block(buf, r, c, pair.at[0, 0], recv, row, sibling).wait_recv()

    def hand_over(gather, j, k):
        buf, recv, along, spread, pair, onward, routed = gather
        block(buf, row_at(j), col_at(k), pair.at[j, k], recv, row, sibling).start()

    def send_plane(gather, k):
        buf, recv, along, spread, pair, onward, routed = gather
        for j in straight + (oblique if routed else []):
            block(buf, row, col_at(k), spread.at[k, j], recv, row_at(j), col).start()
        hand_over(gather, 0, k)

    def relays(gather, j, k):
        buf, recv, along, spread, pair, onward, routed = gather
        copies = []
        if routed:
            targets = []
        elif j // side == 0 and k % 2 == 0:
            targets = [d * side for d in range(1, nrow // side)]
        elif j % side == 0 and k % 2 == 1:
            targets = range(1, side)
        else:
            targets = []
        return [
            block(buf, row_at(j), col_at(k), onward.at[j, k, i], recv, row_at(t), col)
            for i, t in enumerate(targets)
        ]

    def relay(gather, k):
        for j in straight:
            arrived(gather, row_at(j), col_at(k))
            for copy in relays(gather, j, k):
                copy.start()
            hand_over(gather, j, k)

    def send_own(gather):
        buf, recv, along, spread, pair, onward, routed = gather
        for k in range(1, nz):
            block(buf, row, col, along.at[k - 1], recv, row, col_at(k)).start()
        send_plane(gather, 0)

    def pass_on(gather, k):
        arrived(gather, row, col_at(k))
        send_plane(gather, k)

    def hand_over_row(gather, j):
        for k in range(nz):
            arrived(gather, row_at(j), col_at(k))
            hand_over(gather, j, k)

    def sibling_row(gather, j):
        for k in range(nz):
            arrived(gather, row_at(j), lax.rem(z + k, nz) * 2 + (1 - core))

    def drain(gather):
        buf, recv, along, spread, pair, onward, routed = gather
        for k in range(1, nz):
            block(buf, row, col, along.at[k - 1], recv, row, col_at(k)).wait_send()
        for k in range(nz):
            for j in straight + (oblique if routed else []):
                block(buf, row, col_at(k), spread.at[k, j], recv, row_at(j), col).wait_send()
                for copy in relays(gather, j, k):
                    copy.wait_send()
            for j in range(nrow):
                block(buf, row_at(j), col_at(k), pair.at[j, k], recv, row, sibling).wait_send()

    points = (gp,) + tuple(sems_p) + (False,)
    start = (gv,) + tuple(sems_v) + (False,)
    middle = (gs,) + tuple(sems_s) + (True,)

    barrier = pltpu.get_barrier_semaphore()
    for j in range(1, nrow):
        pl.semaphore_signal(barrier, inc=1, device_id=(row_at(j), col), device_id_type=MESH)
    for k in range(1, ncol):
        pl.semaphore_signal(barrier, inc=1, device_id=(row, lax.rem(col + k, ncol)), device_id_type=MESH)

    own = pl.ds(pl.multiple_of(col * high, high), high)
    x = upright(pts_ref[...])
    gp[row, own, :] = side_by_side(x, stacks)
    gv[row, own, :] = side_by_side(upright(vec_ref[...]), stacks)
    pl.semaphore_wait(barrier, nrow + ncol - 2)

    send_own(points)
    send_own(start)

    rate = -KERNEL_SCALE / features * LOG2E
    xf = x.astype(jnp.float32)
    here = jnp.sum(xf * xf, axis=1, keepdims=True) * rate
    blank = jnp.zeros_like(x)
    left = []
    for s in range(per_tile):
        parts = [x if s == t else blank for t in range(per_tile)]
        left.append(jnp.concatenate(parts, axis=1))
    lane = lax.broadcasted_iota(jnp.int32, (8 * per_tile, LANES), 1)
    down = lax.broadcasted_iota(jnp.int32, (8 * per_tile, LANES), 0)
    picks = (lane // features == down // 8).astype(jnp.bfloat16)
    contract = (((1,), (1,)), ((), ()))

    def weights(r):
        for s in range(stacks):
            tile, part = s // per_tile, s % per_tile
            right = gp[r, :, tile * LANES : (tile + 1) * LANES]
            if part == 0:
                wide = right.astype(jnp.float32)
                square = wide * wide
                upper = square.astype(jnp.bfloat16)
                lower = (square - upper.astype(jnp.float32)).astype(jnp.bfloat16)
                there = (
                    lax.dot_general(picks, upper, contract, preferred_element_type=jnp.float32)
                    + lax.dot_general(picks, lower, contract, preferred_element_type=jnp.float32)
                ) * rate
            cross = lax.dot_general(left[part], right, contract, preferred_element_type=jnp.float32)
            power = (cross * (-2.0 * rate) + there[8 * part : 8 * part + 1]) + here
            aff[r, s] = jnp.exp2(power).astype(jnp.bfloat16)

    for k in range(1, nz):
        pass_on(points, k)
        pass_on(start, k)
        relay(points, k - 1)
    relay(points, nz - 1)
    sibling_row(points, 0)
    weights(row)
    for k in range(nz):
        relay(start, k)
    for j in straight:
        sibling_row(points, j)
        weights(row_at(j))
        if j == straight[0]:
            for o in oblique:
                hand_over_row(points, o)
    for j in oblique:
        sibling_row(points, j)
        weights(row_at(j))

    span = gv.shape[2]
    ones = jnp.ones((ncol * high, LANES), jnp.bfloat16)
    acc[...] = jnp.zeros_like(acc)

    def first_row(j):
        sibling_row(start, j)
        r = row_at(j)
        panel = jnp.concatenate([gv[r], ones], axis=1)
        for s in range(stacks):
            acc[s] += jnp.dot(aff[r, s], panel, preferred_element_type=jnp.float32)

    for j in oblique:
        hand_over_row(start, j)
    for j in [0] + straight:
        first_row(j)
    for j in oblique:
        first_row(j)

    product = sum(acc[s][:, s * vectors : (s + 1) * vectors] for s in range(stacks))
    degree = sum(acc[s][:, span : span + vectors] for s in range(stacks))
    scaled = product / degree
    gs[row, own, :] = side_by_side(scaled.astype(jnp.bfloat16), stacks)
    send_own(middle)

    folds = LANES // vectors
    tall = vectors // folds

    def gram_send(step, value):
        part = jnp.dot(value.T, value, precision=HIGHEST, preferred_element_type=jnp.float32) * (1.0 / total)
        gram_col[step, col] = jnp.concatenate([part[f * tall : (f + 1) * tall] for f in range(folds)], axis=1)
        for k in range(1, ncol):
            gram_copy(gram_col, step, col, k - 1, row, lax.rem(col + k, ncol), 0).start()

    def gram_copy(buf, step, slot, k, to_row, to_col, axis):
        return pltpu.make_async_remote_copy(
            src_ref=buf.at[step, slot], dst_ref=buf.at[step, slot],
            send_sem=sems_g[2 * axis].at[step, k], recv_sem=sems_g[2 * axis + 1].at[step, slot],
            device_id=(to_row, to_col), device_id_type=MESH,
        )

    def gram_across(step):
        for k in range(1, ncol):
            slot = lax.rem(col + k, ncol)
            gram_copy(gram_col, step, slot, k - 1, row, slot, 0).wait_recv()
        gram_row[step, row] = sum(gram_col[step, c] for c in range(ncol))
        for j in range(1, nrow):
            gram_copy(gram_row, step, row, j - 1, row_at(j), col, 1).start()

    def gram_whole(step):
        for j in range(1, nrow):
            gram_copy(gram_row, step, row_at(j), j - 1, row_at(j), col, 1).wait_recv()
        flat = sum(gram_row[step, r] for r in range(nrow))
        return jnp.concatenate([flat[:, f * vectors : (f + 1) * vectors] for f in range(folds)], axis=0)

    def gram_drain(step):
        for k in range(1, ncol):
            gram_copy(gram_col, step, col, k - 1, row, lax.rem(col + k, ncol), 0).wait_send()
        for j in range(1, nrow):
            gram_copy(gram_row, step, row, j - 1, row_at(j), col, 1).wait_send()

    for k in range(1, nz):
        pass_on(middle, k)
        relay(middle, k - 1)
    relay(middle, nz - 1)
    mixed = jnp.zeros((span, span), jnp.float32)
    acc[...] = jnp.zeros_like(acc)

    def second_row(j):
        sibling_row(middle, j)
        r = row_at(j)
        for s in range(stacks):
            acc[s, :, :span] += jnp.dot(aff[r, s], gs[r], preferred_element_type=jnp.float32)
        return mixed + jnp.dot(upright(gs[r]), gs[r], preferred_element_type=jnp.float32)

    for j in oblique:
        hand_over_row(middle, j)
    for j in [0] + straight:
        mixed = second_row(j)
    for j in oblique:
        mixed = second_row(j)
    gram = sum(
        mixed[s * vectors : (s + 1) * vectors, s * vectors : (s + 1) * vectors] for s in range(stacks)
    )
    first = inverse_factor(gram * (1.0 / total))
    product = sum(acc[s][:, s * vectors : (s + 1) * vectors] for s in range(stacks))
    scaled = lax.dot_general(
        product / degree, first, contract, precision=HIGHEST, preferred_element_type=jnp.float32
    )
    gram_send(0, scaled)
    drain(points)
    drain(start)
    drain(middle)
    gram_across(0)
    second = inverse_factor(gram_whole(0))
    out_ref[...] = lax.dot_general(second, scaled, contract, precision=HIGHEST, preferred_element_type=jnp.float32)
    gram_drain(0)


def solution(mesh):
    nrow, ncol = mesh.shape["row"], mesh.shape["col"]
    nz = ncol // 2

    def step(points, start_vectors):
        rows, features = points.shape
        vectors = start_vectors.shape[1]
        stacks = packing(rows)
        high = rows // stacks
        wide, span = width(stacks, features), width(stacks, vectors)
        dma = pltpu.SemaphoreType.DMA
        gather = [dma((nrow, ncol)), dma((nz,)), dma((nz, nrow)), dma((nrow, nz)), dma((nrow, nz, square_side(nrow)))]
        tall = vectors * vectors // LANES
        return pl.pallas_call(
            functools.partial(kernel, nrow, ncol, rows * nrow * ncol),
            out_shape=jax.ShapeDtypeStruct((vectors, rows), jnp.float32),
            in_specs=[pl.BlockSpec(memory_space=pltpu.VMEM)] * 2,
            out_specs=pl.BlockSpec(memory_space=pltpu.VMEM),
            scratch_shapes=[
                pltpu.VMEM((nrow, ncol * high, wide), jnp.bfloat16),
                pltpu.VMEM((nrow, ncol * high, span), jnp.bfloat16),
                pltpu.VMEM((nrow, ncol * high, span), jnp.bfloat16),
                pltpu.VMEM((nrow, stacks, rows, ncol * high), jnp.bfloat16),
                pltpu.VMEM((stacks, rows, span + LANES), jnp.float32),
                pltpu.VMEM((1, ncol, tall, LANES), jnp.float32),
                pltpu.VMEM((1, nrow, tall, LANES), jnp.float32),
                gather, gather, gather,
                [dma((1, ncol)), dma((1, ncol)), dma((1, nrow)), dma((1, nrow))],
            ],
            compiler_params=pltpu.CompilerParams(
                collective_id=0, has_side_effects=True, vmem_limit_bytes=56 * 1024 * 1024
            ),
        )(points.T, start_vectors.T).T

    return jax.shard_map(
        step,
        mesh=mesh,
        in_specs=(P(("row", "col"), None), P(("row", "col"), None)),
        out_specs=P(("row", "col"), None),
        check_vma=False,
    )
```
